32 devices in a mesh: tp: 4 (over y, x), dp: 8 (over z, core).
Axes of the slice: x: 2, y: 2, z: 4, core: 2. Of those that a mesh axis runs over, the one named last changes fastest.
Arguments:
- activations: bfloat16 [2, 8192, 8192], P(None, 'dp', 'tp'), may hold values from -72 to 72
- out_grads: bfloat16 [2, 8192, 2048], P(None, 'dp'), may hold values from -2 to 2
- master: float32 [8192, 2, 2048], P(('tp', 'dp')), may hold values from -1.2 to 1.2
- first_moment: float32 [8192, 2, 2048], P(('tp', 'dp')), may hold values from -1.8 to 1.8
- second_moment: float32 [8192, 2, 2048], P(('tp', 'dp')), may hold values from 0.01 to 1
Outputs:
- new_master: float32 [8192, 2, 2048], P(('tp', 'dp'))
- new_first: float32 [8192, 2, 2048], P(('tp', 'dp'))
- new_second: float32 [8192, 2, 2048], P(('tp', 'dp'))
- weights: bfloat16 [8192, 2, 2048], P('tp')
The draws below stay inside these ranges and needn't reach their ends.
All inputs are finite; a program needn't handle non-finite values.
Results may differ from the reference program's by a relative error of at most 0.0004.
Values may be sent and summed in bfloat16 or wider, within the bound.
A program may use at most 192 MiB of HBM per device.

```python
import math
import jax
import jax.numpy as jnp

D = 8192
KVW = 2048
LAYERS = 2
TOKENS = 8192


def shared_signs(key):
    sign_bits = jax.random.randint(jax.random.fold_in(key, 101), (LAYERS, TOKENS), 0, 2)
    return (2 * sign_bits - 1).astype(jnp.float32)


def draw_activations(key, part):
    token_signs = shared_signs(key)
    noise_key = jax.random.fold_in(key, 202)
    along_key = jax.random.fold_in(key, 203)
    noise = jnp.clip(jax.random.normal(noise_key, (LAYERS, TOKENS, D), jnp.float32), -6.0, 6.0)
    direction = jnp.clip(jax.random.normal(along_key, (LAYERS, D), jnp.float32), -3.0, 3.0)
    strength = 8.0
    values = 8.0 * noise + strength * token_signs[:, :, None] * direction[:, None, :]
    return values.astype(jnp.bfloat16)


def draw_out_grads(key, part):
    token_signs = shared_signs(key)
    noise_key = jax.random.fold_in(key, 302)
    along_key = jax.random.fold_in(key, 303)
    noise = jnp.clip(jax.random.normal(noise_key, (LAYERS, TOKENS, KVW), jnp.float32), -6.0, 6.0)
    direction = jnp.clip(jax.random.normal(along_key, (LAYERS, KVW), jnp.float32), -3.0, 3.0)
    values = noise * TOKENS ** (-0.5) + token_signs[:, :, None] * direction[:, None, :] * (1.0 / TOKENS)
    return values.astype(jnp.bfloat16)


def block_scale(own_key, shape, split, smallest, high):
    factor_of = 1.0
    for dim, blocks in split:
        steps = jax.random.uniform(jax.random.fold_in(jax.random.fold_in(own_key, 6), dim), (blocks,), jnp.float32, smallest / len(split), high / len(split))
        factor_of = factor_of * jnp.repeat(jnp.exp(steps), shape[dim] // blocks).reshape((-1,) + (1,) * (len(shape) - 1 - dim))
    return factor_of


def centred(key, dims, width, reach, pieces=(), dtype=jnp.bfloat16):
    values = width * jax.random.normal(key, dims, jnp.float32)
    if pieces:
        values = values * block_scale(key, dims, pieces, -0.22, 0.18)
    return jnp.clip(values, -reach, reach).astype(dtype)


def setup_inputs(seed: int = 0) -> dict:
    keys = jax.random.split(jax.random.key(seed), 6)
    return {
        "activations": draw_activations(jax.random.fold_in(keys[5], 71), 0),
        "out_grads": draw_out_grads(jax.random.fold_in(keys[5], 71), 0),
        "master": centred(keys[2], (D, LAYERS, KVW), 0.2, 1.2, ((0, 32),), jnp.float32),
        "first_moment": centred(keys[3], (D, LAYERS, KVW), 0.3, 1.8, ((0, 32),), jnp.float32),
        "second_moment": jnp.clip(jnp.exp(math.log(1.0) - 4.6051702 * jax.random.uniform(keys[4], (D, LAYERS, KVW), jnp.float32) ** block_scale(keys[4], (D, LAYERS, KVW), ((0, 32),), -0.2, 0.2)), 0.01, 1.0),
    }


beta_first = 0.9
beta_second = 0.95
first_fix = 1.0 - 0.9 ** 10
second_fix = 1.0 - 0.95 ** 10
learn_rate = 0.01
decay_rate = 0.1
epsilon = 1e-08
limit_scale = 2.0

def reference(activations, out_grads, master, first_moment, second_moment):
    grad = jnp.einsum('ltd,ltc->dlc', activations.astype(jnp.float32), out_grads.astype(jnp.float32))
    squares = jnp.sum(grad * grad)
    limit = limit_scale * math.sqrt(D * LAYERS * KVW)
    clip_factor = limit / jnp.maximum(jnp.sqrt(squares), limit)
    clipped = clip_factor * grad
    new_first = beta_first * first_moment + (1.0 - beta_first) * clipped
    new_second = beta_second * second_moment + (1.0 - beta_second) * clipped * clipped
    step_dir = new_first / first_fix / (jnp.sqrt(new_second / second_fix) + epsilon)
    new_master = master - learn_rate * (step_dir + decay_rate * master)
    return (new_master, new_first, new_second, new_master.astype(jnp.bfloat16))
```

```python
import functools
import math

import jax
import jax.numpy as jnp
from jax import lax
from jax.experimental import pallas as pl
from jax.experimental.layout import Layout, with_layout_constraint
from jax.experimental.pallas import tpu as pltpu
from jax.sharding import PartitionSpec as P

beta_first = 0.9
beta_second = 0.95
first_fix = 1.0 - 0.9**10
second_fix = 1.0 - 0.95**10
learn_rate = 0.01
decay_rate = 0.1
epsilon = 1e-08
limit_scale = 2.0
MESH = pl.DeviceIdType.MESH


def total_kernel(n_tp, n_dp, value_ref, total_ref, held, send_sem, recv_sem):
    count = n_tp * n_dp
    me = lax.axis_index("tp") * n_dp + lax.axis_index("dp")

    def device(k):
        other = lax.rem(me + k, count)
        return {"tp": other // n_dp, "dp": lax.rem(other, n_dp)}

    def copy(k, slot):
        return pltpu.make_async_remote_copy(
            src_ref=value_ref,
            dst_ref=held.at[slot],
            send_sem=send_sem.at[k],
            recv_sem=recv_sem.at[k],
            device_id=device(k),
            device_id_type=MESH,
        )

    barrier = pltpu.get_barrier_semaphore()

    @pl.loop(1, count)
    def _(k):
        pl.semaphore_signal(barrier, inc=1, device_id=device(k), device_id_type=MESH)

    pl.semaphore_wait(barrier, count - 1)

    @pl.loop(1, count)
    def _(k):
        copy(k, me).start()

    held[me] = value_ref[...]

    @pl.loop(1, count)
    def _(k):
        copy(k, lax.rem(me - k + count, count)).wait()

    total_ref[...] = jnp.sum(held[...], axis=0)


def device_total(value):
    n_tp, n_dp = lax.axis_size("tp"), lax.axis_size("dp")
    count = n_tp * n_dp
    total = pl.pallas_call(
        functools.partial(total_kernel, n_tp, n_dp),
        out_shape=jax.ShapeDtypeStruct((8, 128), jnp.float32),
        in_specs=[pl.BlockSpec(memory_space=pltpu.VMEM)],
        out_specs=pl.BlockSpec(memory_space=pltpu.VMEM),
        scratch_shapes=[
            pltpu.VMEM((count, 8, 128), jnp.float32),
            pltpu.SemaphoreType.DMA((count,)),
            pltpu.SemaphoreType.DMA((count,)),
        ],
        compiler_params=pltpu.CompilerParams(collective_id=0, has_side_effects=True),
        name="device_total",
    )(jnp.full((8, 128), value, jnp.float32))
    return total[0, 0]


def reduce_rows(activations, out_grads):
    n_dp = lax.axis_size("dp")
    cores = 2 if n_dp % 2 == 0 else 1
    chips = n_dp // cores
    index = lax.axis_index("dp")
    chip, core = index // cores, lax.rem(index, cores)
    layers, tokens, width = activations.shape
    rows = width // n_dp
    top = jnp.max(jnp.abs(activations)).astype(jnp.float32)
    top = top * jnp.max(jnp.abs(out_grads)).astype(jnp.float32)
    bound = jnp.maximum(device_total(tokens * top), 1e-25)
    shrink, grow = 32000.0 / bound, bound / 32000.0

    def pack(x):
        return (x * shrink).astype(jnp.float16)

    def unpack(x):
        return x.astype(jnp.float32) * grow

    swap = [(i, i // cores * cores + (i + 1) % cores) for i in range(n_dp)]
    owns, outs = [], []
    split = activations.reshape(layers, tokens, chips, cores, rows)

    def product(layer, which):
        acts = lax.dynamic_index_in_dim(split[layer], which, 2, keepdims=False)
        acts = acts.reshape(tokens, chips * rows)
        return jnp.einsum("tr,tc->rc", acts, out_grads[layer], preferred_element_type=jnp.float32)

    for layer in range(layers):
        if cores == 2:
            sent = lax.ppermute(pack(product(layer, 1 - core)), "dp", swap)
            outs.append(sent.reshape(chips, rows, -1))
        owns.append(product(layer, core).reshape(chips, rows, -1))

    def block(layer, which):
        value = lax.dynamic_index_in_dim(owns[layer], which, 0, keepdims=False)
        if cores == 2:
            value = value + unpack(lax.dynamic_index_in_dim(outs[layer], which, 0, keepdims=False))
        return value

    running = [None] * layers
    for step in range(chips - 1):
        for layer in range(layers):
            way = 1 if layer % 2 == 0 else -1
            which = lax.rem(chip - way * (1 + step) + chips, chips)
            value = block(layer, which)
            if running[layer] is not None:
                value = value + unpack(running[layer])
            ring = [(i, (i + way * cores) % n_dp) for i in range(n_dp)]
            running[layer] = lax.ppermute(pack(value), "dp", ring)
    done = []
    for layer in range(layers):
        value = block(layer, chip)
        if running[layer] is not None:
            value = value + unpack(running[layer])
        done.append(value)
    return done


def adam_update(grad_own, master, first_moment, second_moment, clip_factor):
    clipped = clip_factor * grad_own
    new_first = beta_first * first_moment + (1.0 - beta_first) * clipped
    new_second = beta_second * second_moment + (1.0 - beta_second) * clipped * clipped
    step_dir = new_first / first_fix / (jnp.sqrt(new_second / second_fix) + epsilon)
    new_master = master - learn_rate * (step_dir + decay_rate * master)
    return (new_master, new_first, new_second)


def on_device(activations, out_grads, master, first_moment, second_moment):
    own_rows = master.shape[0]
    layer_grads = reduce_rows(activations, out_grads)
    sum_squares = device_total(sum(jnp.sum(g * g) for g in layer_grads))
    entries = (
        own_rows * lax.axis_size("tp") * lax.axis_size("dp") * master.shape[1] * master.shape[2]
    )
    limit = limit_scale * math.sqrt(entries)
    clip_factor = limit / jnp.maximum(jnp.sqrt(sum_squares), limit)
    grad_own = with_layout_constraint(jnp.stack(layer_grads, axis=1), Layout((0, 1, 2)))
    new_master, new_first, new_second = adam_update(
        grad_own, master, first_moment, second_moment, clip_factor
    )
    rounded = new_master.astype(jnp.bfloat16)
    tp_rows = lax.all_gather(rounded, "dp", axis=0, tiled=True)
    return (new_master, new_first, new_second, tp_rows)


def solution(mesh):
    return jax.shard_map(
        on_device,
        mesh=mesh,
        in_specs=(
            P(None, "dp", "tp"),
            P(None, "dp", None),
            P(("tp", "dp"), None, None),
            P(("tp", "dp"), None, None),
            P(("tp", "dp"), None, None),
        ),
        out_specs=(
            P(("tp", "dp"), None, None),
            P(("tp", "dp"), None, None),
            P(("tp", "dp"), None, None),
            P("tp", None, None),
        ),
        check_vma=False,
    )
```

```python
import functools
import math

import jax
import jax.numpy as jnp
from jax import lax
from jax.experimental import pallas as pl
from jax.experimental.layout import Layout, with_layout_constraint
from jax.experimental.pallas import tpu as pltpu
from jax.sharding import PartitionSpec as P

beta_first = 0.9
beta_second = 0.95
first_fix = 1.0 - 0.9**10
second_fix = 1.0 - 0.95**10
learn_rate = 0.01
decay_rate = 0.1
epsilon = 1e-08
limit_scale = 2.0
MESH = pl.DeviceIdType.MESH


def total_kernel(n_tp, n_dp, value_ref, total_ref, held, send_sem, recv_sem):
    count = n_tp * n_dp
    me = lax.axis_index("tp") * n_dp + lax.axis_index("dp")

    def device(k):
        other = lax.rem(me + k, count)
        return {"tp": other // n_dp, "dp": lax.rem(other, n_dp)}

    def copy(k, slot):
        return pltpu.make_async_remote_copy(
            src_ref=value_ref,
            dst_ref=held.at[slot],
            send_sem=send_sem.at[k],
            recv_sem=recv_sem.at[k],
            device_id=device(k),
            device_id_type=MESH,
        )

    barrier = pltpu.get_barrier_semaphore()

    @pl.loop(1, count)
    def _(k):
        pl.semaphore_signal(barrier, inc=1, device_id=device(k), device_id_type=MESH)

    pl.semaphore_wait(barrier, count - 1)

    @pl.loop(1, count)
    def _(k):
        copy(k, me).start()

    held[me] = value_ref[...]

    @pl.loop(1, count)
    def _(k):
        copy(k, lax.rem(me - k + count, count)).wait()

    total_ref[0] = jnp.sum(held[...], axis=0)
    total_ref[1] = jnp.sum(held[pl.ds(lax.axis_index("tp") * n_dp, n_dp)], axis=0)


def device_total(value):
    n_tp, n_dp = lax.axis_size("tp"), lax.axis_size("dp")
    count = n_tp * n_dp
    total = pl.pallas_call(
        functools.partial(total_kernel, n_tp, n_dp),
        out_shape=jax.ShapeDtypeStruct((2, 8, 128), jnp.float32),
        in_specs=[pl.BlockSpec(memory_space=pltpu.VMEM)],
        out_specs=pl.BlockSpec(memory_space=pltpu.VMEM),
        scratch_shapes=[
            pltpu.VMEM((count, 8, 128), jnp.float32),
            pltpu.SemaphoreType.DMA((count,)),
            pltpu.SemaphoreType.DMA((count,)),
        ],
        compiler_params=pltpu.CompilerParams(collective_id=0, has_side_effects=True),
        name="device_total",
    )(jnp.full((8, 128), value, jnp.float32))
    return total[0, 0, 0], total[1, 0, 0]


def reduce_rows(activations, out_grads):
    n_dp = lax.axis_size("dp")
    cores = 2 if n_dp % 2 == 0 else 1
    chips = n_dp // cores
    index = lax.axis_index("dp")
    chip, core = index // cores, lax.rem(index, cores)
    layers, tokens, width = activations.shape
    rows = width // n_dp

    def longest(x):
        squares = jnp.sum(jnp.square(x.astype(jnp.float32)), axis=1)
        return jnp.sqrt(jnp.max(squares))

    _, bound = device_total(longest(activations) * longest(out_grads))
    bound = jnp.maximum(1.001 * bound, 1e-25)
    shrink, grow = 250.0 / bound, bound / 250.0

    def pack(x):
        x = x * shrink
        return (x * jnp.abs(x)).astype(jnp.float16)

    def unpack(x):
        x = x.astype(jnp.float32)
        return jnp.sign(x) * jnp.sqrt(jnp.abs(x)) * grow

    swap = [(i, i // cores * cores + (i + 1) % cores) for i in range(n_dp)]
    ways = [1 if layer % 2 == 0 else -1 for layer in range(layers)]
    rings = [[(i, (i + way * cores) % n_dp) for i in range(n_dp)] for way in ways]

    def product(acts, layer, which, half):
        start = (which * cores + half) * rows
        acts = lax.dynamic_slice_in_dim(acts[layer], start, rows, axis=1)
        return jnp.einsum("tr,tc->rc", acts, out_grads[layer], preferred_element_type=jnp.float32)

    def block(acts, layer, step):
        which = lax.rem(chip - ways[layer] * (1 + step) + 2 * chips, chips)
        if cores == 1:
            return product(acts, layer, which, core)
        other = lax.ppermute(pack(product(acts, layer, which, 1 - core)), "dp", swap)
        return product(acts, layer, which, core) + unpack(other)

    values = [block(activations, layer, 0) for layer in range(layers)]
    if chips > 1:
        first = [pack(value) for value in values]
        activations, first = lax.optimization_barrier((activations, first))
        later = [
            [block(activations, layer, step) for layer in range(layers)]
            for step in range(1, chips)
        ]
        running = [lax.ppermute(first[i], "dp", rings[i]) for i in range(layers)]
        for step, blocks in enumerate(later, 1):
            values = [blocks[i] + unpack(running[i]) for i in range(layers)]
            if step < chips - 1:
                running = [lax.ppermute(pack(values[i]), "dp", rings[i]) for i in range(layers)]
    return values


def adam_update(grad_own, master, first_moment, second_moment, clip_factor):
    clipped = clip_factor * grad_own
    new_first = beta_first * first_moment + (1.0 - beta_first) * clipped
    new_second = beta_second * second_moment + (1.0 - beta_second) * clipped * clipped
    step_dir = new_first / first_fix / (jnp.sqrt(new_second / second_fix) + epsilon)
    new_master = master - learn_rate * (step_dir + decay_rate * master)
    return (new_master, new_first, new_second)


def on_device(activations, out_grads, master, first_moment, second_moment):
    own_rows = master.shape[0]
    layer_grads = reduce_rows(activations, out_grads)
    sum_squares, _ = device_total(sum(jnp.sum(g * g) for g in layer_grads))
    entries = (
        own_rows * lax.axis_size("tp") * lax.axis_size("dp") * master.shape[1] * master.shape[2]
    )
    limit = limit_scale * math.sqrt(entries)
    clip_factor = limit / jnp.maximum(jnp.sqrt(sum_squares), limit)
    grad_own = with_layout_constraint(jnp.stack(layer_grads, axis=1), Layout((0, 1, 2)))
    new_master, new_first, new_second = adam_update(
        grad_own, master, first_moment, second_moment, clip_factor
    )
    rounded = new_master.astype(jnp.bfloat16)
    tp_rows = lax.all_gather(rounded, "dp", axis=0, tiled=True)
    return (new_master, new_first, new_second, tp_rows)


def solution(mesh):
    return jax.shard_map(
        on_device,
        mesh=mesh,
        in_specs=(
            P(None, "dp", "tp"),
            P(None, "dp", None),
            P(("tp", "dp"), None, None),
            P(("tp", "dp"), None, None),
            P(("tp", "dp"), None, None),
        ),
        out_specs=(
            P(("tp", "dp"), None, None),
            P(("tp", "dp"), None, None),
            P(("tp", "dp"), None, None),
            P("tp", None, None),
        ),
        check_vma=False,
    )
```

```python
import functools
import math

import jax
import jax.numpy as jnp
from jax import lax
from jax.experimental import pallas as pl
from jax.experimental.layout import Layout, with_layout_constraint
from jax.experimental.pallas import tpu as pltpu
from jax.sharding import PartitionSpec as P

beta_first = 0.9
beta_second = 0.95
first_fix = 1.0 - 0.9**10
second_fix = 1.0 - 0.95**10
learn_rate = 0.01
decay_rate = 0.1
epsilon = 1e-08
limit_scale = 2.0
MESH = pl.DeviceIdType.MESH


def total_kernel(n_tp, n_dp, value_ref, total_ref, held, send_sem, recv_sem):
    count = n_tp * n_dp
    me = lax.axis_index("tp") * n_dp + lax.axis_index("dp")

    def device(k):
        other = lax.rem(me + k, count)
        return {"tp": other // n_dp, "dp": lax.rem(other, n_dp)}

    def copy(k, slot):
        return pltpu.make_async_remote_copy(
            src_ref=value_ref,
            dst_ref=held.at[slot],
            send_sem=send_sem.at[k],
            recv_sem=recv_sem.at[k],
            device_id=device(k),
            device_id_type=MESH,
        )

    barrier = pltpu.get_barrier_semaphore()

    @pl.loop(1, count)
    def _(k):
        pl.semaphore_signal(barrier, inc=1, device_id=device(k), device_id_type=MESH)

    pl.semaphore_wait(barrier, count - 1)

    @pl.loop(1, count)
    def _(k):
        copy(k, me).start()

    held[me] = value_ref[...]

    @pl.loop(1, count)
    def _(k):
        copy(k, lax.rem(me - k + count, count)).wait()

    total_ref[0] = jnp.sum(held[...], axis=0)
    total_ref[1] = jnp.sum(held[pl.ds(lax.axis_index("tp") * n_dp, n_dp)], axis=0)


def device_total(value):
    n_tp, n_dp = lax.axis_size("tp"), lax.axis_size("dp")
    count = n_tp * n_dp
    total = pl.pallas_call(
        functools.partial(total_kernel, n_tp, n_dp),
        out_shape=jax.ShapeDtypeStruct((2, 8, 128), jnp.float32),
        in_specs=[pl.BlockSpec(memory_space=pltpu.VMEM)],
        out_specs=pl.BlockSpec(memory_space=pltpu.VMEM),
        scratch_shapes=[
            pltpu.VMEM((count, 8, 128), jnp.float32),
            pltpu.SemaphoreType.DMA((count,)),
            pltpu.SemaphoreType.DMA((count,)),
        ],
        compiler_params=pltpu.CompilerParams(collective_id=0, has_side_effects=True),
        name="device_total",
    )(jnp.full((8, 128), value, jnp.float32))
    return total[0, 0, 0], total[1, 0, 0]


def reduce_rows(activations, out_grads):
    n_dp = lax.axis_size("dp")
    cores = 2 if n_dp % 2 == 0 else 1
    chips = n_dp // cores
    index = lax.axis_index("dp")
    chip, core = index // cores, lax.rem(index, cores)
    layers, tokens, width = activations.shape
    rows = width // n_dp

    def longest(x):
        squares = jnp.sum(jnp.square(x.astype(jnp.float32)), axis=1)
        return jnp.sqrt(jnp.max(squares))

    _, bound = device_total(longest(activations) * longest(out_grads))
    bound = jnp.maximum(1.001 * bound, 1e-25)
    shrink, grow = 250.0 / bound, bound / 250.0

    def pack(x):
        x = x * shrink
        return (x * jnp.abs(x)).astype(jnp.float16)

    def unpack(x):
        x = x.astype(jnp.float32)
        return jnp.sign(x) * jnp.sqrt(jnp.abs(x)) * grow

    swap = [(i, i // cores * cores + (i + 1) % cores) for i in range(n_dp)]
    ways = [1 if layer % 2 == 0 else -1 for layer in range(layers)]
    rings = [[(i, (i + way * cores) % n_dp) for i in range(n_dp)] for way in ways]

    def product(acts, layer, which, half):
        start = (which * cores + half) * rows
        acts = lax.dynamic_slice_in_dim(acts[layer], start, rows, axis=1)
        return jnp.einsum("tr,tc->rc", acts, out_grads[layer], preferred_element_type=jnp.float32)

    def block(acts, layer, step):
        which = lax.rem(chip - ways[layer] * (1 + step) + 2 * chips, chips)
        if cores == 1:
            return product(acts, layer, which, core)
        other = lax.ppermute(pack(product(acts, layer, which, 1 - core)), "dp", swap)
        return product(acts, layer, which, core) + unpack(other)

    values = [block(activations, layer, 0) for layer in range(layers)]
    if chips > 1:
        first = [pack(value) for value in values]
        activations, first = lax.optimization_barrier((activations, first))
        later = [
            [block(activations, layer, step) for layer in range(layers)]
            for step in range(1, chips)
        ]
        running = [lax.ppermute(first[i], "dp", rings[i]) for i in range(layers)]
        for step, blocks in enumerate(later, 1):
            values = [blocks[i] + unpack(running[i]) for i in range(layers)]
            if step < chips - 1:
                running = [lax.ppermute(pack(values[i]), "dp", rings[i]) for i in range(layers)]
    return values


def adam_update(grad_own, master, first_moment, second_moment, clip_factor):
    clipped = clip_factor * grad_own
    new_first = beta_first * first_moment + (1.0 - beta_first) * clipped
    new_second = beta_second * second_moment + (1.0 - beta_second) * clipped * clipped
    step_dir = new_first / first_fix / (jnp.sqrt(new_second / second_fix) + epsilon)
    new_master = master - learn_rate * (step_dir + decay_rate * master)
    return (new_master, new_first, new_second)


def on_device(activations, out_grads, master, first_moment, second_moment):
    own_rows = master.shape[0]
    layer_grads = reduce_rows(activations, out_grads)
    sum_squares, _ = device_total(sum(jnp.sum(g * g) for g in layer_grads))
    entries = (
        own_rows * lax.axis_size("tp") * lax.axis_size("dp") * master.shape[1] * master.shape[2]
    )
    limit = limit_scale * math.sqrt(entries)
    clip_factor = limit / jnp.maximum(jnp.sqrt(sum_squares), limit)
    grad_own = with_layout_constraint(jnp.stack(layer_grads, axis=1), Layout((0, 1, 2)))
    states = (grad_own, master, first_moment, second_moment)
    cut = own_rows // 2
    head = adam_update(*(x[:cut] for x in states), clip_factor)[0].astype(jnp.bfloat16)
    clip_factor, head = lax.optimization_barrier((clip_factor, head))
    head_rows = lax.all_gather(head, "dp", axis=0)
    new_master, new_first, new_second = adam_update(*states, clip_factor)
    tail = new_master[cut:].astype(jnp.bfloat16)
    tail_rows = lax.all_gather(tail, "dp", axis=0)
    tp_rows = jnp.zeros((lax.axis_size("dp"),) + master.shape, jnp.bfloat16)
    tp_rows = lax.dynamic_update_slice_in_dim(tp_rows, head_rows, 0, 1)
    tp_rows = lax.optimization_barrier(tp_rows)
    tp_rows = lax.dynamic_update_slice_in_dim(tp_rows, tail_rows, cut, 1)
    return (new_master, new_first, new_second, tp_rows.reshape((-1,) + master.shape[1:]))


def solution(mesh):
    return jax.shard_map(
        on_device,
        mesh=mesh,
        in_specs=(
            P(None, "dp", "tp"),
            P(None, "dp", None),
            P(("tp", "dp"), None, None),
            P(("tp", "dp"), None, None),
            P(("tp", "dp"), None, None),
        ),
        out_specs=(
            P(("tp", "dp"), None, None),
            P(("tp", "dp"), None, None),
            P(("tp", "dp"), None, None),
            P("tp", None, None),
        ),
        check_vma=False,
    )
```
